32 devices in a mesh: heads: 2 (over x), cpo: 4 (over z), cp: 4 (over y, core).
Axes of the slice: x: 2, y: 2, z: 4, core: 2. Of those that a mesh axis runs over, the one named last changes fastest.
Arguments:
- queries: bfloat16 [12, 256, 40, 128], P(None, ('cpo', 'cp'), 'heads'), parts along dimension 2
- attn_out: bfloat16 [12, 256, 40, 128], P(None, ('cpo', 'cp'), 'heads'), parts along dimension 2
- grad_out: bfloat16 [12, 256, 40, 128], P(None, ('cpo', 'cp'), 'heads'), parts along dimension 2
- log_sum_exp: float32 [12, 256, 40], P(None, ('cpo', 'cp'), 'heads'), parts along dimension 2
- key_cache: bfloat16 [19456, 8, 128], P(('cpo', 'cp'), 'heads'), parts along dimension 1
- value_cache: bfloat16 [19456, 8, 128], P(('cpo', 'cp'), 'heads'), parts along dimension 1
Outputs:
- output 1: bfloat16 [12, 256, 40, 128], P(None, ('cpo', 'cp'), 'heads'), parts along dimension 2
- output 2: float32 [19456, 8, 128], P(('cpo', 'cp'), 'heads'), parts along dimension 1
- output 3: float32 [19456, 8, 128], P(('cpo', 'cp'), 'heads'), parts along dimension 1
There are 2 independent parts. The reference program is written for one: setup_inputs(seed, part) draws one part's arguments, and reference() takes and returns one part's arrays. A program takes and returns all parts, laid end to end along the dimension named above; each array names one.
All inputs are finite; a program needn't handle non-finite values.
Results may differ from the reference program's by a relative error of at most 0.001.
Values are sent between devices in bfloat16 or wider.
A program may use at most 1 GiB of HBM per device.

```python
import jax
import jax.numpy as jnp
from jax import lax

N_SLICES = 12
SLICE_LEN = 256
PREFIX_BASE = 16384
Q_HEADS = 20
KV_HEADS = 4
HEAD_DIM = 128
ROW_BLOCK = 8


def slice_lse(queries_f, keys_f, slice_idx):
    group_size = Q_HEADS // KV_HEADS
    softmax_scale = HEAD_DIM ** -0.5
    limit_len = PREFIX_BASE + (slice_idx + 1) * SLICE_LEN
    key_part = keys_f[:limit_len]
    key_pos = jnp.arange(limit_len)
    n_blocks = SLICE_LEN // ROW_BLOCK
    q_blocks = queries_f.reshape(n_blocks, ROW_BLOCK, KV_HEADS, group_size, HEAD_DIM)
    row_starts = PREFIX_BASE + slice_idx * SLICE_LEN + ROW_BLOCK * jnp.arange(n_blocks)

    def one_block(operand):
        q_blk, row_start = operand
        scores = jnp.einsum('rhgd,khd->rhgk', q_blk, key_part) * softmax_scale
        q_pos = row_start + jnp.arange(ROW_BLOCK)
        visible = (key_pos[None, :] <= q_pos[:, None])[:, None, None, :]
        scores = jnp.where(visible, scores, -jnp.inf)
        return jax.nn.logsumexp(scores, axis=-1).reshape(ROW_BLOCK, Q_HEADS)

    return lax.map(one_block, (q_blocks, row_starts)).reshape(SLICE_LEN, Q_HEADS)


def setup_inputs(seed: int = 0, part: int = 0) -> dict:
    base_key = jax.random.fold_in(jax.random.key(seed), part)
    key_q, key_k, key_v, key_o, key_g = jax.random.split(base_key, 5)
    total_len = PREFIX_BASE + N_SLICES * SLICE_LEN
    row_shape = (N_SLICES, SLICE_LEN, Q_HEADS, HEAD_DIM)
    cache_shape = (total_len, KV_HEADS, HEAD_DIM)
    queries = jax.random.normal(key_q, row_shape, jnp.float32).astype(jnp.bfloat16)
    key_cache = jax.random.normal(key_k, cache_shape, jnp.float32).astype(jnp.bfloat16)
    value_cache = jax.random.normal(key_v, cache_shape, jnp.float32).astype(jnp.bfloat16)
    out_val = jax.random.normal(key_o, row_shape, jnp.float32)
    grad_out = (0.1 * out_val + jax.random.normal(key_g, row_shape, jnp.float32)).astype(jnp.bfloat16)
    attn_out = out_val.astype(jnp.bfloat16)
    queries_f = queries.astype(jnp.float32)
    keys_f = key_cache.astype(jnp.float32)
    log_sum_exp = jnp.stack([slice_lse(queries_f[slice_idx], keys_f, slice_idx) for slice_idx in range(N_SLICES)])
    return {'queries': queries, 'attn_out': attn_out, 'grad_out': grad_out, 'log_sum_exp': log_sum_exp, 'key_cache': key_cache, 'value_cache': value_cache}


def reference(queries, attn_out, grad_out, log_sum_exp, key_cache, value_cache):
    group_size = Q_HEADS // KV_HEADS
    softmax_scale = HEAD_DIM ** -0.5
    total_len = PREFIX_BASE + N_SLICES * SLICE_LEN
    n_blocks = SLICE_LEN // ROW_BLOCK
    blk_shape = (n_blocks, ROW_BLOCK, KV_HEADS, group_size)
    keys_f = key_cache.astype(jnp.float32)
    values_f = value_cache.astype(jnp.float32)
    row_delta = jnp.sum(grad_out.astype(jnp.float32) * attn_out.astype(jnp.float32), axis=-1)
    grad_key = jnp.zeros((total_len, KV_HEADS, HEAD_DIM), jnp.float32)
    grad_value = jnp.zeros((total_len, KV_HEADS, HEAD_DIM), jnp.float32)
    dq_list = []
    for slice_idx in reversed(range(N_SLICES)):
        limit_len = PREFIX_BASE + (slice_idx + 1) * SLICE_LEN
        key_part = keys_f[:limit_len]
        value_part = values_f[:limit_len]
        key_pos = jnp.arange(limit_len)
        operands = (
            queries[slice_idx].astype(jnp.float32).reshape(blk_shape + (HEAD_DIM,)),
            grad_out[slice_idx].astype(jnp.float32).reshape(blk_shape + (HEAD_DIM,)),
            log_sum_exp[slice_idx].reshape(blk_shape),
            row_delta[slice_idx].reshape(blk_shape),
            PREFIX_BASE + slice_idx * SLICE_LEN + ROW_BLOCK * jnp.arange(n_blocks),
        )

        def one_block(carry_acc, operand):
            key_acc, value_acc = carry_acc
            q_blk, g_blk, lse_blk, delta_blk, row_start = operand
            scores = jnp.einsum('rhgd,khd->rhgk', q_blk, key_part) * softmax_scale
            q_pos = row_start + jnp.arange(ROW_BLOCK)
            visible = (key_pos[None, :] <= q_pos[:, None])[:, None, None, :]
            attn_prob = jnp.where(visible, jnp.exp(scores - lse_blk[..., None]), 0.0)
            prob_bf = attn_prob.astype(jnp.bfloat16).astype(jnp.float32)
            value_acc = value_acc + jnp.einsum('rhgk,rhgd->khd', prob_bf, g_blk)
            grad_prob = jnp.einsum('rhgd,khd->rhgk', g_blk, value_part)
            grad_scores = attn_prob * (grad_prob - delta_blk[..., None])
            grad_scores = grad_scores.astype(jnp.bfloat16).astype(jnp.float32)
            dq_blk = jnp.einsum('rhgk,khd->rhgd', grad_scores, key_part) * softmax_scale
            key_acc = key_acc + softmax_scale * jnp.einsum('rhgk,rhgd->khd', grad_scores, q_blk)
            return (key_acc, value_acc), dq_blk.astype(jnp.bfloat16)

        start_acc = (grad_key[:limit_len], grad_value[:limit_len])
        (key_acc, value_acc), dq_blocks = lax.scan(one_block, start_acc, operands)
        grad_key = lax.dynamic_update_slice(grad_key, key_acc, (0, 0, 0))
        grad_value = lax.dynamic_update_slice(grad_value, value_acc, (0, 0, 0))
        dq_list.append(dq_blocks.reshape(SLICE_LEN, Q_HEADS, HEAD_DIM))
    grad_query = jnp.stack(dq_list[::-1])
    return grad_query, grad_key, grad_value
```

```python
import functools

import jax
import jax.numpy as jnp
from jax import lax
from jax.experimental import pallas as pl
from jax.experimental.pallas import tpu as pltpu
from jax.sharding import PartitionSpec as P

CP_AXES = ('cpo', 'cp')
LOG2E = 1.4426950408889634
KEY_BLOCK = 256
N_CHUNKS = 3


def key_kernel(n_cp, key_rows, *refs):
    parts = refs[:n_cp]
    k_ref, kt_ref, vt_ref, kv_scr, sems = refs[n_cp:]
    me = lax.axis_index('cp')
    copies = []
    for s in range(n_cp):
        start = pl.multiple_of((me ^ s) * key_rows, 64)
        copy = pltpu.make_async_copy(parts[s], kv_scr.at[:, pl.ds(start, key_rows), :], sems.at[s])
        copy.start()
        copies.append(copy)
    for copy in copies:
        copy.wait()
    k_ref[...] = kv_scr[0]
    n_blocks = n_cp * key_rows // KEY_BLOCK

    def step(b, carry):
        rows = pl.ds(pl.multiple_of(b * KEY_BLOCK, KEY_BLOCK), KEY_BLOCK)
        kt_ref[:, rows] = kv_scr[0, rows, :].T
        vt_ref[:, rows] = kv_scr[1, rows, :].T
        return carry

    lax.fori_loop(0, n_blocks, step, 0)


def grad_kernel(first_slice, n_in, n_pl, n_pref_last, last, n_cp, scale, *refs):
    (own, up1, up2, up3, dn1, dn2, dn3, stat, qpos, k_ref, kt_ref, vt_ref) = refs[:12]
    idx = 12
    if not first_slice:
        dk_in, dv_in = refs[idx:idx + 2]
        idx += 2
    dq_ref, dk_out, dv_out = refs[idx:idx + 3]
    (qg_scr, qt_scr, gt_scr, l_scr, d_scr, p_scr, ds_scr, dk_scr, dv_scr, sems) = refs[idx + 3:]
    n_slices = own.shape[0]
    piece = own.shape[2]
    rows = n_pl * piece
    n_blocks = kt_ref.shape[1] // KEY_BLOCK
    z = lax.axis_index('cpo')
    j = pl.program_id(0)
    ups = (None, up1, up2, up3)
    dns = (None, dn1, dn2, dn3)

    def fetch(jj, start):
        slot = lax.rem(jj, 2)

        def go(src, k):
            copy = pltpu.make_async_copy(src.at[jj], qg_scr.at[slot, :, pl.ds(k * piece, piece), :], sems.at[slot, k])
            if start:
                copy.start()
            else:
                copy.wait()

        go(own, 0)
        for k in range(1, n_pl):
            if start:
                @pl.when(z >= k)
                def _():
                    go(ups[k], k)

                @pl.when(z < k)
                def _():
                    go(dns[n_pl - k], k)
            else:
                go(ups[k], k)

    @pl.when(j == 0)
    def _():
        fetch(j, True)
        if first_slice:
            dk_scr[...] = jnp.zeros_like(dk_scr)
            dv_scr[...] = jnp.zeros_like(dv_scr)
        else:
            dk_scr[...] = dk_in[...]
            dv_scr[...] = dv_in[...]

    fetch(j, False)

    @pl.when(j + 1 < n_slices)
    def _():
        fetch(j + 1, True)

    slot = lax.rem(j, 2)
    q_scr = qg_scr.at[slot, 0]
    g_scr = qg_scr.at[slot, 1]
    qt_scr[...] = q_scr[...].T
    gt_scr[...] = g_scr[...].T
    stat_t = stat[0].T
    l_scr[...] = jnp.broadcast_to(stat_t[:, 0:1] * LOG2E, l_scr.shape)
    d_scr[...] = jnp.broadcast_to(stat_t[:, 1:2], d_scr.shape)

    sub = 256

    def cols_of(b):
        return pl.ds(pl.multiple_of(b * KEY_BLOCK, KEY_BLOCK), KEY_BLOCK)

    def scores(r, kt, vt, masked):
        rr = pl.ds(r * sub, sub)
        s = jnp.dot(q_scr[rr, :], kt, preferred_element_type=jnp.float32)
        dp = jnp.dot(g_scr[rr, :], vt, preferred_element_type=jnp.float32)
        return s, dp

    def probs(r, s, dp, masked):
        rr = pl.ds(r * sub, sub)
        lb = l_scr[rr, :]
        db = d_scr[rr, :]
        lb = jnp.concatenate([lb, lb], axis=1)
        db = jnp.concatenate([db, db], axis=1)
        p = jnp.exp2(s * (scale * LOG2E) - lb)
        if masked:
            pos = qpos[rr, :]
            pos = jnp.concatenate([pos, pos], axis=1)
            key = lax.broadcasted_iota(jnp.int32, (sub, KEY_BLOCK), 1)
            p = jnp.where(key <= pos, p, 0.0)
        return p.astype(jnp.bfloat16), (p * (dp - db)).astype(jnp.bfloat16)

    def query_grad(r, ds, kk, masked):
        rr = pl.ds(r * sub, sub)
        dq = jnp.dot(ds, kk, preferred_element_type=jnp.float32)
        if masked:
            dq_ref[0, rr, :] = dq
        else:
            dq_ref[0, rr, :] += dq

    def add(acc, x):
        return x if acc is None else acc + x

    n_sub = rows // sub

    def block(b, masked):
        cols = cols_of(b)
        kt = kt_ref[:, cols]
        vt = vt_ref[:, cols]
        kk = k_ref[cols, :]
        acc_v = acc_k = None
        held = None
        for r in range(n_sub + 1):
            if r < n_sub:
                s, dp = scores(r, kt, vt, masked)
            if held is not None:
                q = pl.ds((r - 1) * sub, sub)
                p, ds = held
                acc_v = add(acc_v, jnp.dot(gt_scr[:, q], p, preferred_element_type=jnp.float32))
                acc_k = add(acc_k, jnp.dot(qt_scr[:, q], ds, preferred_element_type=jnp.float32))
                query_grad(r - 1, ds, kk, masked)
            if r < n_sub:
                held = probs(r, s, dp, masked)
        dv_scr[:, cols] += acc_v
        dk_scr[:, cols] += acc_k

    first_block = jnp.where(z == n_pl - 1, n_pref_last + n_in + j, n_blocks - 1)
    block(first_block, True)

    def step(b, carry):
        block(b, False)
        return carry

    lax.fori_loop(0, first_block, step, 0)

    @pl.when(j == n_slices - 1)
    def _():
        if last:
            def out(b, carry):
                cols = pl.ds(pl.multiple_of(b * KEY_BLOCK, KEY_BLOCK), KEY_BLOCK)
                dk_out[cols, :] = dk_scr[:, cols].T * scale
                dv_out[cols, :] = dv_scr[:, cols].T
                return carry

            lax.fori_loop(0, n_blocks, out, 0)
        else:
            dk_out[...] = dk_scr[...]
            dv_out[...] = dv_scr[...]


def solution(mesh):
    n_cpo = mesh.shape['cpo']
    n_cp = mesh.shape['cp']
    row_spec = P(None, CP_AXES, 'heads', None)
    stat_spec = P(None, CP_AXES, 'heads')
    key_spec = P(CP_AXES, 'heads', None)

    def local_grads(queries, attn_out, grad_out, log_sum_exp, key_cache, value_cache):
        n_slices, rows_dev, q_heads, head_dim = queries.shape
        key_rows, kv_heads, _ = key_cache.shape
        group = q_heads // kv_heads
        slice_len = rows_dev * n_cp * n_cpo
        plane_keys = key_rows * n_cp
        prefix = plane_keys * n_cpo - n_slices * slice_len
        n_pref_last = (prefix - plane_keys * (n_cpo - 1)) // KEY_BLOCK
        scale = head_dim ** -0.5
        piece = n_cp * rows_dev * group
        rows = n_cpo * piece
        per = n_slices // N_CHUNKS
        z = lax.axis_index('cpo')
        c = lax.axis_index('cp')

        def xor_pairs(s):
            return [(i, i ^ s) for i in range(n_cp)]

        def exchange(x, axis):
            out = []
            for s in range(n_cp):
                part = lax.dynamic_index_in_dim(x, c ^ s, axis, keepdims=False)
                out.append(part if s == 0 else lax.ppermute(part, 'cp', xor_pairs(s)))
            return out

        def line(x):
            ups, dns = [], []
            u = d = x
            for k in range(1, n_cpo):
                u = lax.ppermute(u, 'cpo', [(i, i + 1) for i in range(k - 1, n_cpo - 1)])
                d = lax.ppermute(d, 'cpo', [(i, i - 1) for i in range(1, n_cpo - k + 1)])
                ups.append(u)
                dns.append(d)
            return ups, dns

        delta = jnp.sum(grad_out.astype(jnp.float32) * attn_out.astype(jnp.float32), axis=-1)
        stats = jnp.stack([log_sum_exp, delta], axis=1).reshape(n_slices, 2, rows_dev, kv_heads, group)

        qg = jnp.stack([queries, grad_out], axis=1).reshape(n_slices, 2, rows_dev, kv_heads, group, head_dim)
        qg = jnp.transpose(qg, (3, 0, 1, 2, 4, 5)).reshape(kv_heads, n_slices, 2, rows_dev * group, head_dim)
        chunks = []
        stat_x = exchange(stats.transpose(3, 0, 1, 2, 4).reshape(kv_heads, n_slices, 2, rows_dev * group), 0)
        stat_own = jnp.concatenate(stat_x, axis=2)
        for g in range(N_CHUNKS):
            parts = exchange(qg[:, g * per:(g + 1) * per], 0)
            own = jnp.concatenate(parts, axis=2)
            ups, dns = line(own)
            chunks.append((own, ups, dns))
            if g == 0:
                s_up, s_dn = line(stat_own)
                kv = jnp.transpose(jnp.stack([key_cache, value_cache]), (2, 0, 1, 3))
                kv_parts = exchange(kv, 0)

        stat_list = [stat_own] + [jnp.where(z >= k, s_up[k - 1], s_dn[n_cpo - k - 1]) for k in range(1, n_cpo)]
        stat_all = jnp.concatenate(stat_list, axis=2)
        stat_all = jnp.concatenate([stat_all, jnp.zeros((n_slices, 6, rows), jnp.float32)], axis=1)

        any_spec = pl.BlockSpec(memory_space=pl.ANY)
        vmem = pl.BlockSpec(memory_space=pltpu.VMEM)
        bf = jnp.bfloat16
        k_all, kt_all, vt_all = pl.pallas_call(
            functools.partial(key_kernel, n_cp, key_rows),
            out_shape=[
                jax.ShapeDtypeStruct((plane_keys, head_dim), bf),
                jax.ShapeDtypeStruct((head_dim, plane_keys), bf),
                jax.ShapeDtypeStruct((head_dim, plane_keys), bf),
            ],
            in_specs=[any_spec] * n_cp,
            out_specs=[vmem] * 3,
            scratch_shapes=[pltpu.VMEM((2, plane_keys, head_dim), bf), pltpu.SemaphoreType.DMA((n_cp,))],
            compiler_params=pltpu.CompilerParams(vmem_limit_bytes=32 * 1024 * 1024),
            name='keys',
        )(*kv_parts)

        r = jnp.arange(rows)
        plane = (z - r // piece) % n_cpo
        src = (r % piece) // (rows_dev * group)
        tok = plane * n_cp * rows_dev + (c ^ src) * rows_dev + (r % (rows_dev * group)) // group
        tok = jnp.where(z == n_cpo - 1, tok, slice_len)
        qpos = jnp.broadcast_to(tok[:, None], (rows, 128)).astype(jnp.int32)

        dk = dv = None
        dq_own = []
        order = list(reversed(range(N_CHUNKS)))
        order = list(range(N_CHUNKS))
        for n, g in enumerate(order):
            own, ups, dns = chunks[g]
            first, last = n == 0, n == N_CHUNKS - 1
            acc_in = [] if first else [dk, dv]
            acc_shape = (plane_keys, head_dim) if last else (head_dim, plane_keys)
            full = lambda shape: pl.BlockSpec(shape, lambda j: (0,) * len(shape))
            dq_part, dk, dv = pl.pallas_call(
                functools.partial(grad_kernel, first, g * per, n_cpo, n_pref_last, last, n_cp, scale),
                grid=(per,),
                out_shape=[
                    jax.ShapeDtypeStruct((per, rows, head_dim), jnp.float32),
                    jax.ShapeDtypeStruct(acc_shape, jnp.float32),
                    jax.ShapeDtypeStruct(acc_shape, jnp.float32),
                ],
                in_specs=[any_spec] * 7 + [pl.BlockSpec((1, 8, rows), lambda j: (j, 0, 0))] + [vmem] * 4 + [vmem] * len(acc_in),
                out_specs=[pl.BlockSpec((1, rows, head_dim), lambda j: (j, 0, 0))] + [vmem] * 2,
                scratch_shapes=[
                    pltpu.VMEM((2, 2, rows, head_dim), bf),
                    pltpu.VMEM((head_dim, rows), bf),
                    pltpu.VMEM((head_dim, rows), bf),
                    pltpu.VMEM((rows, 128), jnp.float32),
                    pltpu.VMEM((rows, 128), jnp.float32),
                    pltpu.VMEM((rows, KEY_BLOCK), bf),
                    pltpu.VMEM((rows, KEY_BLOCK), bf),
                    pltpu.VMEM((head_dim, plane_keys), jnp.float32),
                    pltpu.VMEM((head_dim, plane_keys), jnp.float32),
                    pltpu.SemaphoreType.DMA((2, n_cpo)),
                ],
                compiler_params=pltpu.CompilerParams(vmem_limit_bytes=48 * 1024 * 1024),
                cost_estimate=pl.CostEstimate(flops=10 * per * rows * plane_keys * head_dim * 2, bytes_accessed=20_000_000, transcendentals=0),
                name='grads',
            )(own, *ups, *dns, stat_all[g * per:(g + 1) * per], qpos, k_all, kt_all, vt_all, *acc_in)

            part = dq_part.reshape(per, n_cpo, piece, head_dim)

            def target(t):
                return lax.dynamic_index_in_dim(part, (z - t) % n_cpo, 1, keepdims=False)

            up = target(z + n_cpo - 1)
            dn = target(z - (n_cpo - 1))
            for s in range(1, n_cpo):
                up = lax.ppermute(up, 'cpo', [(i, i + 1) for i in range(s)])
                dn = lax.ppermute(dn, 'cpo', [(i, i - 1) for i in range(n_cpo - s, n_cpo)])
                if s < n_cpo - 1:
                    up = up + target(z + n_cpo - 1 - s)
                    dn = dn + target(z - (n_cpo - 1 - s))
            dq = ((target(z) + up + dn) * scale).astype(bf)
            dq = dq.reshape(per, n_cp, rows_dev * group, head_dim)
            dq_own.append(dq)

        def exchange_back(get, x_out, axis):
            for s in range(n_cp):
                part = get(s)
                if s:
                    part = lax.ppermute(part, 'cp', xor_pairs(s))
                x_out = lax.dynamic_update_index_in_dim(x_out, part, c ^ s, axis)
            return x_out

        def key_out(x):
            x = x.reshape(n_cp, key_rows, head_dim)
            get = lambda s: lax.dynamic_index_in_dim(x, c ^ s, 0, keepdims=False)
            return jnp.transpose(exchange_back(get, jnp.zeros((kv_heads, key_rows, head_dim), jnp.float32), 0), (1, 0, 2))

        dq_all = jnp.concatenate(dq_own, axis=0)
        dq_heads = exchange_back(lambda s: dq_all[:, s], jnp.zeros((kv_heads, n_slices, rows_dev * group, head_dim), bf), 0)
        dq_heads = dq_heads.reshape(kv_heads, n_slices, rows_dev, group, head_dim)
        grad_query = jnp.transpose(dq_heads, (1, 2, 0, 3, 4)).reshape(queries.shape)
        return grad_query, key_out(dk), key_out(dv)

    return jax.shard_map(local_grads, mesh=mesh, in_specs=(row_spec, row_spec, row_spec, stat_spec, key_spec, key_spec), out_specs=(row_spec, key_spec, key_spec), check_vma=False)
```

```python
import functools

import jax
import jax.numpy as jnp
from jax import lax
from jax.experimental import pallas as pl
from jax.experimental.pallas import tpu as pltpu
from jax.sharding import PartitionSpec as P

CP_AXES = ('cpo', 'cp')
MESH = pl.DeviceIdType.MESH
LOG2E = 1.4426950408889634
KEY_BLOCK = 256
SUB = 256
AHEAD = 4
FIRST = 2


def attention_kernel(n_pl, n_cp, n_pref_last, scale, *refs):
    (qg, kv, st, qpos, dq_out, dk_out, dv_out) = refs[:7]
    (gat, kv_scr, kt_scr, vt_scr, st_scr, dqp, ru, rd, dqb, dk_scr, dv_scr, dko, dvo, qt_scr, gt_scr, l_scr, d_scr) = refs[7:24]
    (q_s, q_r, kv_s, kv_r, st_s, st_r, sz_s, sz_r, ag_s, ag_r, rs_s, rs_r, dq_s, dq_r, dk_s, dk_r) = refs[24:]
    n_slices = gat.shape[0]
    rows = gat.shape[2]
    piece = rows // n_pl
    part = piece // n_cp
    key_rows = kv.shape[2]
    n_blocks = kv_scr.shape[1] // KEY_BLOCK
    far = n_pl - 1
    z = lax.axis_index('cpo')
    c = lax.axis_index('cp')

    def mate(s):
        return {0: c, 1: c + 1 - 2 * lax.rem(c, 2), 2: lax.rem(c + 2, n_cp), 3: n_cp - 1 - c}[s]

    def remote(src, dst, send, recv, **where):
        return pltpu.make_async_remote_copy(src_ref=src, dst_ref=dst, send_sem=send, recv_sem=recv, device_id=where, device_id_type=MESH)

    def slot(k):
        return pl.ds(k * piece, piece)

    barrier = pltpu.get_barrier_semaphore()
    for s in range(1, n_cp):
        pl.semaphore_signal(barrier, inc=1, device_id={'cp': mate(s)}, device_id_type=MESH)
    for step in (1, n_pl - 1):
        pl.semaphore_signal(barrier, inc=1, device_id={'cpo': lax.rem(z + step, n_pl)}, device_id_type=MESH)
    pl.semaphore_wait(barrier, n_cp + 1)

    def q_copy(j, s):
        dst = gat.at[j, :, pl.ds(s * part, part), :]
        if s == 0:
            return pltpu.make_async_copy(qg.at[c, j], dst, q_r.at[j, 0])
        return remote(qg.at[mate(s), j], dst, q_s.at[s], q_r.at[j, s], cp=mate(s))

    def q_start(j, carry):
        for s in range(n_cp):
            q_copy(j, s).start()
        return carry

    def key_place(who):
        return kv_scr.at[:, pl.ds(pl.multiple_of(who * key_rows, 64), key_rows), :]

    def kv_copy(s):
        if s == 0:
            return pltpu.make_async_copy(kv.at[c], key_place(c), kv_r.at[0])
        return remote(kv.at[mate(s)], key_place(c), kv_s.at[s], kv_r.at[s], cp=mate(s))

    def st_copy(s):
        if s == 0:
            return pltpu.make_async_copy(st.at[c], st_scr.at[0, 0], st_r.at[0])
        return remote(st.at[mate(s)], st_scr.at[0, s], st_s.at[s], st_r.at[s], cp=mate(s))

    lax.fori_loop(0, FIRST, q_start, 0)
    for s in range(n_cp):
        st_copy(s).start()
    for s in range(n_cp):
        kv_copy(s).start()
    lax.fori_loop(FIRST, n_slices, q_start, 0)

    def ups(h):
        return (z < far) & (z >= h - 1)

    def downs(h):
        return (z >= 1) & (z <= n_pl - h)

    def q_hop(j, h, up):
        a, b = (h - 1, h) if up else ((n_pl - h + 1) % n_pl, n_pl - h)
        d = 0 if up else 1
        return remote(gat.at[j, :, slot(a), :], gat.at[j, :, slot(b), :], ag_s.at[d, h - 1], ag_r.at[j, b], cpo=z + 1 if up else z - 1)

    def st_hop(h, up):
        a, b = (h - 1, h) if up else ((n_pl - h + 1) % n_pl, n_pl - h)
        d = 0 if up else 1
        return remote(st_scr.at[a], st_scr.at[b], sz_s.at[d, h - 1], sz_r.at[b], cpo=z + 1 if up else z - 1)

    def send_hop(make, h):
        @pl.when(ups(h))
        def _():
            make(h, True).start()

        @pl.when(downs(h))
        def _():
            make(h, False).start()

    def wait_hop(make, h):
        @pl.when(z >= h)
        def _():
            make(h, True).wait_recv()

        @pl.when(z <= far - h)
        def _():
            make(h, False).wait_recv()

    def ag_first(j):
        for s in range(n_cp):
            copy = q_copy(j, s)
            copy.wait() if s == 0 else copy.wait_recv()
        send_hop(lambda h, up: q_hop(j, h, up), 1)

    def ag_next(j, h):
        wait_hop(lambda h, up: q_hop(j, h, up), h - 1)
        send_hop(lambda h, up: q_hop(j, h, up), h)

    def ag_service(j):
        for h in range(1, n_pl):
            jj = j + AHEAD - (h - 1)

            @pl.when((jj < n_slices) & (jj >= 0))
            def _():
                ag_first(jj) if h == 1 else ag_next(jj, h)

    def rs_copy(j, s, up):
        k = s if up else n_pl - s
        d = 0 if up else 1
        dst = (ru if up else rd).at[j, s - 1]
        return remote(dqp.at[j, slot(k), :], dst, rs_s.at[d, s - 1], rs_r.at[d, j, s - 1], cpo=z + 1 if up else z - 1)

    def rs_step(j, s):
        if s > 1:
            @pl.when((z >= 1) & (z <= s - 1))
            def _():
                rs_copy(j, s - 1, True).wait_recv()
                dqp[j, slot(s), :] += ru[j, s - 2]

            @pl.when((z >= n_pl - s) & (z <= far - 1))
            def _():
                rs_copy(j, s - 1, False).wait_recv()
                dqp[j, slot(n_pl - s), :] += rd[j, s - 2]

        @pl.when(z <= s - 1)
        def _():
            rs_copy(j, s, True).start()

        @pl.when(z >= n_pl - s)
        def _():
            rs_copy(j, s, False).start()

    def dq_copy(j, s):
        src = dqb.at[j, pl.ds(s * part, part), :]
        if s == 0:
            return pltpu.make_async_copy(src, dq_out.at[c, j], dq_r.at[0])
        return remote(src, dq_out.at[c, j], dq_s.at[s], dq_r.at[s], cp=mate(s))

    def rs_final(j):
        @pl.when(z >= 1)
        def _():
            rs_copy(j, far, True).wait_recv()
            dqp[j, slot(0), :] += ru[j, far - 1]

        @pl.when(z <= far - 1)
        def _():
            rs_copy(j, far, False).wait_recv()
            dqp[j, slot(0), :] += rd[j, far - 1]

        dqb[j] = (dqp[j, slot(0), :] * scale).astype(jnp.bfloat16)
        for s in range(n_cp):
            dq_copy(j, s).start()

    def rs_service(j):
        for s in range(1, n_pl + 1):
            jj = j - s

            @pl.when((jj >= 0) & (jj < n_slices))
            def _():
                rs_step(jj, s) if s < n_pl else rs_final(jj)

    def compute(j):
        cols16 = [st_scr[k, s, pl.ds(2 * j, 2), :] for k in range(n_pl) for s in range(n_cp)]
        stat_t = jnp.concatenate(cols16, axis=0).T
        for i in range(n_pl * n_cp):
            rr = pl.ds(i * part, part)
            l_scr[rr, :] = jnp.broadcast_to(stat_t[:part, 2 * i:2 * i + 1] * LOG2E, (part, 128))
            d_scr[rr, :] = jnp.broadcast_to(stat_t[:part, 2 * i + 1:2 * i + 2], (part, 128))
        qt_scr[...] = gat[j, 0].T
        gt_scr[...] = gat[j, 1].T

        def scores(r, kt, vt):
            rr = pl.ds(r * SUB, SUB)
            s = jnp.dot(gat[j, 0, rr, :], kt, preferred_element_type=jnp.float32)
            dp = jnp.dot(gat[j, 1, rr, :], vt, preferred_element_type=jnp.float32)
            return s, dp

        def probs(r, s, dp, masked):
            rr = pl.ds(r * SUB, SUB)
            lb = l_scr[rr, :]
            db = d_scr[rr, :]
            lb = jnp.concatenate([lb, lb], axis=1)
            db = jnp.concatenate([db, db], axis=1)
            p = jnp.exp2(s * (scale * LOG2E) - lb)
            if masked:
                pos = qpos[rr, :]
                pos = jnp.concatenate([pos, pos], axis=1)
                key = lax.broadcasted_iota(jnp.int32, (SUB, KEY_BLOCK), 1)
                p = jnp.where(key <= pos, p, 0.0)
            return p.astype(jnp.bfloat16), (p * (dp - db)).astype(jnp.bfloat16)

        def block(b, masked):
            cols = pl.ds(pl.multiple_of(b * KEY_BLOCK, KEY_BLOCK), KEY_BLOCK)
            kt = kt_scr[:, cols]
            vt = vt_scr[:, cols]
            kk = kv_scr[0, cols, :]
            acc_v = acc_k = held = None
            n_sub = rows // SUB
            for r in range(n_sub + 1):
                if r < n_sub:
                    s, dp = scores(r, kt, vt)
                if held is not None:
                    q = pl.ds((r - 1) * SUB, SUB)
                    p, ds = held
                    av = jnp.dot(gt_scr[:, q], p, preferred_element_type=jnp.float32)
                    ak = jnp.dot(qt_scr[:, q], ds, preferred_element_type=jnp.float32)
                    acc_v = av if acc_v is None else acc_v + av
                    acc_k = ak if acc_k is None else acc_k + ak
                    dq = jnp.dot(ds, kk, preferred_element_type=jnp.float32)
                    if masked:
                        dqp[j, q, :] = dq
                    else:
                        dqp[j, q, :] += dq
                if r < n_sub:
                    held = probs(r, s, dp, masked)
            dv_scr[:, cols] += acc_v
            dk_scr[:, cols] += acc_k

        first_block = lax.div(z, far) * (n_pref_last + j - (n_blocks - 1)) + n_blocks - 1
        block(first_block, True)

        def step(b, carry):
            block(b, False)
            return carry

        lax.fori_loop(0, first_block, step, 0)

    dk_scr[...] = jnp.zeros_like(dk_scr)
    dv_scr[...] = jnp.zeros_like(dv_scr)
    for j in range(FIRST):
        ag_first(j)
    for s in range(n_cp):
        copy = st_copy(s)
        copy.wait() if s == 0 else copy.wait_recv()
    send_hop(st_hop, 1)
    for h in range(2, n_pl):
        for j in range(FIRST):
            ag_next(j, h)
        wait_hop(st_hop, h - 1)
        send_hop(st_hop, h)
    for s in range(n_cp):
        copy = kv_copy(s)
        copy.wait() if s == 0 else copy.wait_recv()

    def turn(b, carry):
        cols = pl.ds(pl.multiple_of(b * KEY_BLOCK, KEY_BLOCK), KEY_BLOCK)
        kt_scr[:, cols] = kv_scr[0, cols, :].T
        vt_scr[:, cols] = kv_scr[1, cols, :].T
        return carry

    lax.fori_loop(0, n_blocks, turn, 0)
    wait_hop(st_hop, far)

    for h in range(1, n_pl):
        for j in range(FIRST, AHEAD - (h - 1)):
            if j < n_slices:
                ag_first(j) if h == 1 else ag_next(j, h)

    def slice_step(j, carry):
        ag_service(j)
        rs_service(j)
        wait_hop(lambda h, up: q_hop(j, h, up), far)
        compute(j)
        return carry

    lax.fori_loop(0, n_slices, slice_step, 0)
    rs_service(n_slices)

    def home(src, out, s, n):
        place = src.at[pl.ds(pl.multiple_of((mate(s)) * key_rows, 64), key_rows), :]
        if s == 0:
            return pltpu.make_async_copy(place, out.at[c], dk_r.at[n, 0])
        return remote(place, out.at[c], dk_s.at[n, s], dk_r.at[n, s], cp=mate(s))

    def turn_back(acc, out, factor):
        def go(b, carry):
            cols = pl.ds(pl.multiple_of(b * KEY_BLOCK, KEY_BLOCK), KEY_BLOCK)
            out[cols, :] = acc[:, cols].T * factor
            return carry

        lax.fori_loop(0, n_blocks, go, 0)

    pairs = ((dv_scr, dvo, dv_out, 1.0), (dk_scr, dko, dk_out, scale))
    for n, (acc, held, out, factor) in enumerate(pairs):
        turn_back(acc, held, factor)
        for s in range(n_cp):
            home(held, out, (s + 1) % n_cp, n).start()

    def flush(j, carry):
        rs_service(j)
        return carry

    lax.fori_loop(n_slices + 1, n_slices + n_pl, flush, 0)

    for s in range(n_cp):
        whole = dqb.at[:, pl.ds(s * part, part), :]
        if s == 0:
            pltpu.make_async_copy(whole, dq_out.at[c], dq_r.at[0]).wait()
        else:
            remote(whole, dq_out.at[mate(s)], dq_s.at[s], dq_r.at[s], cp=mate(s)).wait()
            remote(qg.at[mate(s)], gat.at[:, :, pl.ds(s * part, part), :], q_s.at[s], q_r.at[0, s], cp=mate(s)).wait_send()
            kv_copy(s).wait_send()
            st_copy(s).wait_send()
        for n, (acc, held, out, factor) in enumerate(pairs):
            home(held, out, s, n).wait()
    for h in range(1, n_pl):
        for up in (True, False):
            cond = ups(h) if up else downs(h)

            @pl.when(cond)
            def _():
                d = 0 if up else 1
                whole = gat.at[:, :, slot(0), :]
                remote(whole, whole, ag_s.at[d, h - 1], ag_r.at[0, 1], cpo=z + 1 if up else z - 1).wait_send()
                st_hop(h, up).wait_send()

            cond = (z <= h - 1) if up else (z >= n_pl - h)

            @pl.when(cond)
            def _():
                d = 0 if up else 1
                whole = dqp.at[:, slot(0), :]
                remote(whole, whole, rs_s.at[d, h - 1], rs_r.at[d, 0, 0], cpo=z + 1 if up else z - 1).wait_send()


def solution(mesh):
    n_cpo = mesh.shape['cpo']
    n_cp = mesh.shape['cp']
    row_spec = P(None, CP_AXES, 'heads', None)
    stat_spec = P(None, CP_AXES, 'heads')
    key_spec = P(CP_AXES, 'heads', None)

    def local_grads(queries, attn_out, grad_out, log_sum_exp, key_cache, value_cache):
        n_slices, rows_dev, q_heads, head_dim = queries.shape
        key_rows, kv_heads, _ = key_cache.shape
        group = q_heads // kv_heads
        slice_len = rows_dev * n_cp * n_cpo
        plane_keys = key_rows * n_cp
        prefix = plane_keys * n_cpo - n_slices * slice_len
        n_pref_last = (prefix - plane_keys * (n_cpo - 1)) // KEY_BLOCK
        scale = head_dim ** -0.5
        part = rows_dev * group
        piece = n_cp * part
        rows = n_cpo * piece
        bf, f32 = jnp.bfloat16, jnp.float32
        z = lax.axis_index('cpo')
        c = lax.axis_index('cp')

        delta = jnp.sum(grad_out.astype(f32) * attn_out.astype(f32), axis=-1)
        st = jnp.stack([log_sum_exp, delta], axis=1).reshape(n_slices, 2, rows_dev, kv_heads, group)
        st = st.transpose(3, 0, 1, 2, 4).reshape(kv_heads, n_slices * 2, part)
        st = jnp.pad(st, ((0, 0), (0, -(n_slices * 2) % 8), (0, 128 - part)))
        qg = jnp.stack([queries, grad_out], axis=1).reshape(n_slices, 2, rows_dev, kv_heads, group, head_dim)
        qg = jnp.transpose(qg, (3, 0, 1, 2, 4, 5)).reshape(kv_heads, n_slices, 2, part, head_dim)
        kv = jnp.transpose(jnp.stack([key_cache, value_cache]), (2, 0, 1, 3))

        r = jnp.arange(rows)
        plane = (z - r // piece) % n_cpo
        tok = plane * n_cp * rows_dev + (c ^ ((r % piece) // part)) * rows_dev + (r % part) // group
        tok = jnp.where(z == n_cpo - 1, tok, slice_len)
        qpos = jnp.broadcast_to(tok[:, None], (rows, 128)).astype(jnp.int32)

        any_spec = pl.BlockSpec(memory_space=pl.ANY)
        vmem = pl.BlockSpec(memory_space=pltpu.VMEM)
        dma = pltpu.SemaphoreType.DMA
        dq, dk, dv = pl.pallas_call(
            functools.partial(attention_kernel, n_cpo, n_cp, n_pref_last, scale),
            out_shape=[
                jax.ShapeDtypeStruct((kv_heads, n_slices, part, head_dim), bf),
                jax.ShapeDtypeStruct((kv_heads, key_rows, head_dim), f32),
                jax.ShapeDtypeStruct((kv_heads, key_rows, head_dim), f32),
            ],
            in_specs=[any_spec] * 3 + [vmem],
            out_specs=[any_spec] * 3,
            scratch_shapes=[
                pltpu.VMEM((n_slices, 2, rows, head_dim), bf),
                pltpu.VMEM((2, plane_keys, head_dim), bf),
                pltpu.VMEM((head_dim, plane_keys), bf),
                pltpu.VMEM((head_dim, plane_keys), bf),
                pltpu.VMEM((n_cpo, n_cp) + st.shape[1:], f32),
                pltpu.VMEM((n_slices, rows, head_dim), f32),
                pltpu.VMEM((n_slices, n_cpo - 1, piece, head_dim), f32),
                pltpu.VMEM((n_slices, n_cpo - 1, piece, head_dim), f32),
                pltpu.VMEM((n_slices, piece, head_dim), bf),
                pltpu.VMEM((head_dim, plane_keys), f32),
                pltpu.VMEM((head_dim, plane_keys), f32),
                pltpu.VMEM((plane_keys, head_dim), f32),
                pltpu.VMEM((plane_keys, head_dim), f32),
                pltpu.VMEM((head_dim, rows), bf),
                pltpu.VMEM((head_dim, rows), bf),
                pltpu.VMEM((rows, 128), f32),
                pltpu.VMEM((rows, 128), f32),
                dma((n_cp,)), dma((n_slices, n_cp)),
                dma((n_cp,)), dma((n_cp,)),
                dma((n_cp,)), dma((n_cp,)),
                dma((2, n_cpo - 1)), dma((n_cpo,)),
                dma((2, n_cpo - 1)), dma((n_slices, n_cpo)),
                dma((2, n_cpo - 1)), dma((2, n_slices, n_cpo - 1)),
                dma((n_cp,)), dma((n_cp,)),
                dma((2, n_cp)), dma((2, n_cp)),
            ],
            compiler_params=pltpu.CompilerParams(vmem_limit_bytes=63 * 1024 * 1024, collective_id=0, has_side_effects=True),
            name='attention_backward',
        )(qg, kv, st, qpos)

        dq = dq.reshape(kv_heads, n_slices, rows_dev, group, head_dim)
        grad_query = jnp.transpose(dq, (1, 2, 0, 3, 4)).reshape(queries.shape)
        return grad_query, jnp.transpose(dk, (1, 0, 2)), jnp.transpose(dv, (1, 0, 2))

    return jax.shard_map(local_grads, mesh=mesh, in_specs=(row_spec, row_spec, row_spec, stat_spec, key_spec, key_spec), out_specs=(row_spec, key_spec, key_spec), check_vma=False)
```

```python
import functools

import jax
import jax.numpy as jnp
from jax import lax
from jax.experimental import pallas as pl
from jax.experimental.pallas import tpu as pltpu
from jax.sharding import PartitionSpec as P

CP_AXES = ('cpo', 'cp')
MESH = pl.DeviceIdType.MESH
LOG2E = 1.4426950408889634
KEY_BLOCK = 256
SUB = 256
AHEAD = 4
FIRST = 2


def attention_kernel(n_pl, n_cp, n_pref_last, scale, *refs):
    (qg, kv, st, qpos, dq_out, dk_out, dv_out) = refs[:7]
    (gat, kv_scr, kt_scr, vt_scr, st_scr, dqp, ru, rd, dqb, dk_scr, dv_scr, dko, dvo, qt_scr, gt_scr, l_scr, d_scr) = refs[7:24]
    (q_s, q_r, kv_s, kv_r, st_s, st_r, sz_s, sz_r, ag_s, ag_r, rs_s, rs_r, dq_s, dq_r, dk_s, dk_r) = refs[24:]
    n_slices = gat.shape[0]
    rows = gat.shape[2]
    piece = rows // n_pl
    part = piece // n_cp
    key_rows = kv.shape[2]
    n_blocks = kv_scr.shape[1] // KEY_BLOCK
    far = n_pl - 1
    z = lax.axis_index('cpo')
    c = lax.axis_index('cp')

    def mate(s):
        return {0: c, 1: c + 1 - 2 * lax.rem(c, 2), 2: lax.rem(c + 2, n_cp), 3: n_cp - 1 - c}[s]

    def remote(src, dst, send, recv, **where):
        return pltpu.make_async_remote_copy(src_ref=src, dst_ref=dst, send_sem=send, recv_sem=recv, device_id=where, device_id_type=MESH)

    def slot(k):
        return pl.ds(k * piece, piece)

    barrier = pltpu.get_barrier_semaphore()
    for s in range(1, n_cp):
        pl.semaphore_signal(barrier, inc=1, device_id={'cp': mate(s)}, device_id_type=MESH)
    for step in (1, n_pl - 1):
        pl.semaphore_signal(barrier, inc=1, device_id={'cpo': lax.rem(z + step, n_pl)}, device_id_type=MESH)
    pl.semaphore_wait(barrier, n_cp + 1)

    def q_copy(j, s):
        dst = gat.at[j, :, pl.ds(s * part, part), :]
        if s == 0:
            return pltpu.make_async_copy(qg.at[c, j], dst, q_r.at[j, 0])
        return remote(qg.at[mate(s), j], dst, q_s.at[s], q_r.at[j, s], cp=mate(s))

    def q_start(j, carry):
        for s in range(n_cp):
            q_copy(j, s).start()
        return carry

    def key_place(who):
        return kv_scr.at[:, pl.ds(pl.multiple_of(who * key_rows, 64), key_rows), :]

    def kv_copy(s):
        if s == 0:
            return pltpu.make_async_copy(kv.at[c], key_place(c), kv_r.at[0])
        return remote(kv.at[mate(s)], key_place(c), kv_s.at[s], kv_r.at[s], cp=mate(s))

    def st_copy(s):
        if s == 0:
            return pltpu.make_async_copy(st.at[c], st_scr.at[0, 0], st_r.at[0])
        return remote(st.at[mate(s)], st_scr.at[0, s], st_s.at[s], st_r.at[s], cp=mate(s))

    lax.fori_loop(0, FIRST, q_start, 0)
    for s in range(n_cp):
        st_copy(s).start()
    for s in range(n_cp):
        kv_copy(s).start()
    lax.fori_loop(FIRST, n_slices, q_start, 0)

    def ups(h):
        return (z < far) & (z >= h - 1)

    def downs(h):
        return (z >= 1) & (z <= n_pl - h)

    def q_hop(j, h, up):
        a, b = (h - 1, h) if up else ((n_pl - h + 1) % n_pl, n_pl - h)
        d = 0 if up else 1
        return remote(gat.at[j, :, slot(a), :], gat.at[j, :, slot(b), :], ag_s.at[d, h - 1], ag_r.at[j, b], cpo=z + 1 if up else z - 1)

    def st_hop(h, up):
        a, b = (h - 1, h) if up else ((n_pl - h + 1) % n_pl, n_pl - h)
        d = 0 if up else 1
        return remote(st_scr.at[a], st_scr.at[b], sz_s.at[d, h - 1], sz_r.at[b], cpo=z + 1 if up else z - 1)

    def send_hop(make, h):
        @pl.when(ups(h))
        def _():
            make(h, True).start()

        @pl.when(downs(h))
        def _():
            make(h, False).start()

    def wait_hop(make, h):
        @pl.when(z >= h)
        def _():
            make(h, True).wait_recv()

        @pl.when(z <= far - h)
        def _():
            make(h, False).wait_recv()

    def ag_first(j):
        for s in range(n_cp):
            copy = q_copy(j, s)
            copy.wait() if s == 0 else copy.wait_recv()
        send_hop(lambda h, up: q_hop(j, h, up), 1)

    def ag_next(j, h):
        wait_hop(lambda h, up: q_hop(j, h, up), h - 1)
        send_hop(lambda h, up: q_hop(j, h, up), h)

    def ag_service(t, due):
        for h in range(1, n_pl):
            jj = t + AHEAD - (h - 1)

            @pl.when(due & (jj < n_slices))
            def _():
                ag_first(jj) if h == 1 else ag_next(jj, h)

    def rs_copy(j, s, up):
        k = s if up else n_pl - s
        d = 0 if up else 1
        dst = (ru if up else rd).at[j, s - 1]
        return remote(dqp.at[j, slot(k), :], dst, rs_s.at[d, s - 1], rs_r.at[d, j, s - 1], cpo=z + 1 if up else z - 1)

    def rs_step(j, s):
        if s > 1:
            @pl.when((z >= 1) & (z <= s - 1))
            def _():
                rs_copy(j, s - 1, True).wait_recv()
                dqp[j, slot(s), :] += ru[j, s - 2]

            @pl.when((z >= n_pl - s) & (z <= far - 1))
            def _():
                rs_copy(j, s - 1, False).wait_recv()
                dqp[j, slot(n_pl - s), :] += rd[j, s - 2]

        @pl.when(z <= s - 1)
        def _():
            rs_copy(j, s, True).start()

        @pl.when(z >= n_pl - s)
        def _():
            rs_copy(j, s, False).start()

    def dq_copy(j, s):
        src = dqb.at[j, pl.ds(s * part, part), :]
        if s == 0:
            return pltpu.make_async_copy(src, dq_out.at[c, j], dq_r.at[0])
        return remote(src, dq_out.at[c, j], dq_s.at[s], dq_r.at[s], cp=mate(s))

    def rs_final(j):
        @pl.when(z >= 1)
        def _():
            rs_copy(j, far, True).wait_recv()
            dqp[j, slot(0), :] += ru[j, far - 1]

        @pl.when(z <= far - 1)
        def _():
            rs_copy(j, far, False).wait_recv()
            dqp[j, slot(0), :] += rd[j, far - 1]

        dqb[j] = (dqp[j, slot(0), :] * scale).astype(jnp.bfloat16)
        for s in range(n_cp):
            dq_copy(j, s).start()

    def rs_service(u, due, low, high):
        for s in range(1, n_pl + 1):
            jj = u - s

            @pl.when(due & (jj >= low) & (jj < high))
            def _():
                rs_step(jj, s) if s < n_pl else rs_final(jj)

    def compute(j, low, high, fresh):
        @pl.when(fresh)
        def _():
            dqp[j] = jnp.zeros(dqp.shape[1:], jnp.float32)

        cols16 = [st_scr[k, s, pl.ds(2 * j, 2), :] for k in range(n_pl) for s in range(n_cp)]
        stat_t = jnp.concatenate(cols16, axis=0).T
        for i in range(n_pl * n_cp):
            rr = pl.ds(i * part, part)
            l_scr[rr, :] = jnp.broadcast_to(stat_t[:part, 2 * i:2 * i + 1] * LOG2E, (part, 128))
            d_scr[rr, :] = jnp.broadcast_to(stat_t[:part, 2 * i + 1:2 * i + 2], (part, 128))
        qt_scr[...] = gat[j, 0].T
        gt_scr[...] = gat[j, 1].T

        def scores(r, kt, vt):
            rr = pl.ds(r * SUB, SUB)
            s = jnp.dot(gat[j, 0, rr, :], kt, preferred_element_type=jnp.float32)
            dp = jnp.dot(gat[j, 1, rr, :], vt, preferred_element_type=jnp.float32)
            return s, dp

        def probs(r, s, dp, masked):
            rr = pl.ds(r * SUB, SUB)
            lb = l_scr[rr, :]
            db = d_scr[rr, :]
            lb = jnp.concatenate([lb, lb], axis=1)
            db = jnp.concatenate([db, db], axis=1)
            p = jnp.exp2(s * (scale * LOG2E) - lb)
            if masked:
                pos = qpos[rr, :]
                pos = jnp.concatenate([pos, pos], axis=1)
                key = lax.broadcasted_iota(jnp.int32, (SUB, KEY_BLOCK), 1)
                p = jnp.where(key <= pos, p, 0.0)
            return p.astype(jnp.bfloat16), (p * (dp - db)).astype(jnp.bfloat16)

        def block(b, masked):
            cols = pl.ds(pl.multiple_of(b * KEY_BLOCK, KEY_BLOCK), KEY_BLOCK)
            kt = kt_scr[:, cols]
            vt = vt_scr[:, cols]
            kk = kv_scr[0, cols, :]
            acc_v = acc_k = held = None
            n_sub = rows // SUB
            for r in range(n_sub + 1):
                if r < n_sub:
                    s, dp = scores(r, kt, vt)
                if held is not None:
                    q = pl.ds((r - 1) * SUB, SUB)
                    p, ds = held
                    av = jnp.dot(gt_scr[:, q], p, preferred_element_type=jnp.float32)
                    ak = jnp.dot(qt_scr[:, q], ds, preferred_element_type=jnp.float32)
                    acc_v = av if acc_v is None else acc_v + av
                    acc_k = ak if acc_k is None else acc_k + ak
                    dq = jnp.dot(ds, kk, preferred_element_type=jnp.float32)
                    dqp[j, q, :] += dq
                if r < n_sub:
                    held = probs(r, s, dp, masked)
            dv_scr[:, cols] += acc_v
            dk_scr[:, cols] += acc_k

        edge = lax.div(z, far) * (n_pref_last + j - (n_blocks - 1)) + n_blocks - 1

        def step(b, carry):
            block(b, False)
            return carry

        lax.fori_loop(low, lax.min(high, edge), step, 0)

        @pl.when((edge >= low) & (edge < high))
        def _():
            block(edge, True)

    dk_scr[...] = jnp.zeros_like(dk_scr)
    dv_scr[...] = jnp.zeros_like(dv_scr)
    for j in range(FIRST):
        ag_first(j)
    for s in range(n_cp):
        copy = st_copy(s)
        copy.wait() if s == 0 else copy.wait_recv()
    send_hop(st_hop, 1)
    for h in range(2, n_pl):
        for j in range(FIRST):
            ag_next(j, h)
        wait_hop(st_hop, h - 1)
        send_hop(st_hop, h)
    y = lax.div(c, 2)
    own = (y * ((n_blocks + 1) // 2), n_blocks // 2 + y * (n_blocks - n_blocks // 2))
    other = ((1 - y) * (n_blocks // 2), n_blocks - y * (n_blocks // 2))

    def turn(b, carry):
        cols = pl.ds(pl.multiple_of(b * KEY_BLOCK, KEY_BLOCK), KEY_BLOCK)
        kt_scr[:, cols] = kv_scr[0, cols, :].T
        vt_scr[:, cols] = kv_scr[1, cols, :].T
        return carry

    kv_copy(0).wait()
    kv_copy(1).wait_recv()
    lax.fori_loop(own[0], own[1], turn, 0)
    wait_hop(st_hop, far)

    def home(src, out, s, n):
        place = src.at[pl.ds(pl.multiple_of(mate(s) * key_rows, 64), key_rows), :]
        if s == 0:
            return pltpu.make_async_copy(place, out.at[c], dk_r.at[n, 0])
        return remote(place, out.at[c], dk_s.at[n, s], dk_r.at[n, s], cp=mate(s))

    pairs = ((dv_scr, dvo, dv_out, 1.0), (dk_scr, dko, dk_out, scale))

    def go_home(span, mates):
        for n, (acc, held, out, factor) in enumerate(pairs):
            def turn_back(b, carry):
                cols = pl.ds(pl.multiple_of(b * KEY_BLOCK, KEY_BLOCK), KEY_BLOCK)
                held[cols, :] = acc[:, cols].T * factor
                return carry

            lax.fori_loop(span[0], span[1], turn_back, 0)
            for s in mates:
                home(held, out, s, n).start()

    half = n_slices // 2

    def item(i, carry):
        early = i < 2 * half
        late = i >= half + n_slices
        j = jnp.where(i < 2, i, jnp.where(i < 4, i - 2, jnp.where(early, lax.div(i, 2), jnp.where(late, i - n_slices, i - half))))
        is_own = jnp.where(i < 2, 1, jnp.where(i < 4, 0, jnp.where(early, 1 - lax.rem(i, 2), jnp.where(late, 1, 0))))
        is_first = jnp.where(i < 2, 1, jnp.where(i < 4, 0, jnp.where(early, 1 - lax.rem(i, 2), jnp.where(late, 0, 1))))
        low = is_own * own[0] + (1 - is_own) * other[0]
        high = is_own * own[1] + (1 - is_own) * other[1]
        even = lax.rem(i, 2) == 0

        for h in range(1, n_pl):
            for jj in range(FIRST, min(AHEAD - (h - 1), n_slices)):
                @pl.when(i == 1)
                def _():
                    ag_first(jj) if h == 1 else ag_next(jj, h)

        ag_service(jnp.where(i < 8, lax.div(i, 2) - 1, i - 5), ((i >= 2) & even) | (i > 8))

        @pl.when(i == 2)
        def _():
            for s in range(2, n_cp):
                kv_copy(s).wait_recv()
            lax.fori_loop(other[0], other[1], turn, 0)

        rs_service(
            jnp.where(i <= 2 * half, lax.div(i, 2), i - half),
            (i == 3) | ((i >= 4) & (i <= 2 * half) & even) | ((i > 2 * half) & (i < 2 * half + n_pl)), 0, half)
        rs_service(i - n_slices, i > half + n_slices, half, n_slices)

        @pl.when(i == half + n_slices)
        def _():
            go_home(other, (2, 3))

        @pl.when(is_first == 1)
        def _():
            wait_hop(lambda h, up: q_hop(j, h, up), far)

        compute(j, low, high, is_first == 1)
        return carry

    lax.fori_loop(0, 2 * n_slices, item, 0)
    rs_service(n_slices, z >= 0, half, n_slices)
    go_home(own, (1, 0))

    def flush(u, carry):
        rs_service(u, u >= 0, half, n_slices)
        return carry

    lax.fori_loop(n_slices + 1, n_slices + n_pl, flush, 0)

    for s in range(n_cp):
        whole = dqb.at[:, pl.ds(s * part, part), :]
        if s == 0:
            pltpu.make_async_copy(whole, dq_out.at[c], dq_r.at[0]).wait()
        else:
            remote(whole, dq_out.at[mate(s)], dq_s.at[s], dq_r.at[s], cp=mate(s)).wait()
            remote(qg.at[mate(s)], gat.at[:, :, pl.ds(s * part, part), :], q_s.at[s], q_r.at[0, s], cp=mate(s)).wait_send()
            kv_copy(s).wait_send()
            st_copy(s).wait_send()
        for n, (acc, held, out, factor) in enumerate(pairs):
            home(held, out, s, n).wait()
    for h in range(1, n_pl):
        for up in (True, False):
            cond = ups(h) if up else downs(h)

            @pl.when(cond)
            def _():
                d = 0 if up else 1
                whole = gat.at[:, :, slot(0), :]
                remote(whole, whole, ag_s.at[d, h - 1], ag_r.at[0, 1], cpo=z + 1 if up else z - 1).wait_send()
                st_hop(h, up).wait_send()

            cond = (z <= h - 1) if up else (z >= n_pl - h)

            @pl.when(cond)
            def _():
                d = 0 if up else 1
                whole = dqp.at[:, slot(0), :]
                remote(whole, whole, rs_s.at[d, h - 1], rs_r.at[d, 0, 0], cpo=z + 1 if up else z - 1).wait_send()


def solution(mesh):
    n_cpo = mesh.shape['cpo']
    n_cp = mesh.shape['cp']
    row_spec = P(None, CP_AXES, 'heads', None)
    stat_spec = P(None, CP_AXES, 'heads')
    key_spec = P(CP_AXES, 'heads', None)

    def local_grads(queries, attn_out, grad_out, log_sum_exp, key_cache, value_cache):
        n_slices, rows_dev, q_heads, head_dim = queries.shape
        key_rows, kv_heads, _ = key_cache.shape
        group = q_heads // kv_heads
        slice_len = rows_dev * n_cp * n_cpo
        plane_keys = key_rows * n_cp
        prefix = plane_keys * n_cpo - n_slices * slice_len
        n_pref_last = (prefix - plane_keys * (n_cpo - 1)) // KEY_BLOCK
        scale = head_dim ** -0.5
        part = rows_dev * group
        piece = n_cp * part
        rows = n_cpo * piece
        bf, f32 = jnp.bfloat16, jnp.float32
        z = lax.axis_index('cpo')
        c = lax.axis_index('cp')

        delta = jnp.sum(grad_out.astype(f32) * attn_out.astype(f32), axis=-1)
        st = jnp.stack([log_sum_exp, delta], axis=1).reshape(n_slices, 2, rows_dev, kv_heads, group)
        st = st.transpose(3, 0, 1, 2, 4).reshape(kv_heads, n_slices * 2, part)
        st = jnp.pad(st, ((0, 0), (0, -(n_slices * 2) % 8), (0, 128 - part)))
        qg = jnp.stack([queries, grad_out], axis=1).reshape(n_slices, 2, rows_dev, kv_heads, group, head_dim)
        qg = jnp.transpose(qg, (3, 0, 1, 2, 4, 5)).reshape(kv_heads, n_slices, 2, part, head_dim)
        kv = jnp.transpose(jnp.stack([key_cache, value_cache]), (2, 0, 1, 3))

        r = jnp.arange(rows)
        plane = (z - r // piece) % n_cpo
        tok = plane * n_cp * rows_dev + (c ^ ((r % piece) // part)) * rows_dev + (r % part) // group
        tok = jnp.where(z == n_cpo - 1, tok, slice_len)
        qpos = jnp.broadcast_to(tok[:, None], (rows, 128)).astype(jnp.int32)

        any_spec = pl.BlockSpec(memory_space=pl.ANY)
        vmem = pl.BlockSpec(memory_space=pltpu.VMEM)
        dma = pltpu.SemaphoreType.DMA
        dq, dk, dv = pl.pallas_call(
            functools.partial(attention_kernel, n_cpo, n_cp, n_pref_last, scale),
            out_shape=[
                jax.ShapeDtypeStruct((kv_heads, n_slices, part, head_dim), bf),
                jax.ShapeDtypeStruct((kv_heads, key_rows, head_dim), f32),
                jax.ShapeDtypeStruct((kv_heads, key_rows, head_dim), f32),
            ],
            in_specs=[any_spec] * 3 + [vmem],
            out_specs=[any_spec] * 3,
            scratch_shapes=[
                pltpu.VMEM((n_slices, 2, rows, head_dim), bf),
                pltpu.VMEM((2, plane_keys, head_dim), bf),
                pltpu.VMEM((head_dim, plane_keys), bf),
                pltpu.VMEM((head_dim, plane_keys), bf),
                pltpu.VMEM((n_cpo, n_cp) + st.shape[1:], f32),
                pltpu.VMEM((n_slices, rows, head_dim), f32),
                pltpu.VMEM((n_slices, n_cpo - 1, piece, head_dim), f32),
                pltpu.VMEM((n_slices, n_cpo - 1, piece, head_dim), f32),
                pltpu.VMEM((n_slices, piece, head_dim), bf),
                pltpu.VMEM((head_dim, plane_keys), f32),
                pltpu.VMEM((head_dim, plane_keys), f32),
                pltpu.VMEM((plane_keys, head_dim), f32),
                pltpu.VMEM((plane_keys, head_dim), f32),
                pltpu.VMEM((head_dim, rows), bf),
                pltpu.VMEM((head_dim, rows), bf),
                pltpu.VMEM((rows, 128), f32),
                pltpu.VMEM((rows, 128), f32),
                dma((n_cp,)), dma((n_slices, n_cp)),
                dma((n_cp,)), dma((n_cp,)),
                dma((n_cp,)), dma((n_cp,)),
                dma((2, n_cpo - 1)), dma((n_cpo,)),
                dma((2, n_cpo - 1)), dma((n_slices, n_cpo)),
                dma((2, n_cpo - 1)), dma((2, n_slices, n_cpo - 1)),
                dma((n_cp,)), dma((n_cp,)),
                dma((2, n_cp)), dma((2, n_cp)),
            ],
            compiler_params=pltpu.CompilerParams(vmem_limit_bytes=63 * 1024 * 1024, collective_id=0, has_side_effects=True),
            name='attention_backward',
        )(qg, kv, st, qpos)

        dq = dq.reshape(kv_heads, n_slices, rows_dev, group, head_dim)
        grad_query = jnp.transpose(dq, (1, 2, 0, 3, 4)).reshape(queries.shape)
        return grad_query, jnp.transpose(dk, (1, 0, 2)), jnp.transpose(dv, (1, 0, 2))

    return jax.shard_map(local_grads, mesh=mesh, in_specs=(row_spec, row_spec, row_spec, stat_spec, key_spec, key_spec), out_specs=(row_spec, key_spec, key_spec), check_vma=False)
```

```python
import functools

import jax
import jax.numpy as jnp
from jax import lax
from jax.experimental import pallas as pl
from jax.experimental.pallas import tpu as pltpu
from jax.sharding import PartitionSpec as P

CP_AXES = ('cpo', 'cp')
MESH = pl.DeviceIdType.MESH
LOG2E = 1.4426950408889634
KEY_BLOCK = 256
SUB = 256
AHEAD = 4
TOGETHER = 3
FIRST = 2


def attention_kernel(n_pl, n_cp, n_pref_last, scale, *refs):
    (q_in, g_in, k_in, v_in, st, qpos, dq_out, dk_out, dv_out) = refs[:9]
    (gat, kv_scr, kt_scr, vt_scr, st_scr, dqp, ru, rd, dqb, dk_scr, dv_scr, dko, dvo, turned, l_scr, d_scr) = refs[9:25]
    (q_s, q_r, kv_s, kv_r, st_s, st_r, sz_s, sz_r, ag_s, ag_r, rs_s, rs_r, dq_s, dq_r, dk_s, dk_r) = refs[25:]
    n_slices = gat.shape[0]
    rows = gat.shape[2]
    piece = rows // n_pl
    part = piece // n_cp
    key_rows = k_in.shape[1]
    n_blocks = kv_scr.shape[1] // KEY_BLOCK
    far = n_pl - 1
    z = lax.axis_index('cpo')
    c = lax.axis_index('cp')

    def mate(s):
        return {0: c, 1: c + 1 - 2 * lax.rem(c, 2), 2: lax.rem(c + 2, n_cp), 3: n_cp - 1 - c}[s]

    def remote(src, dst, send, recv, **where):
        return pltpu.make_async_remote_copy(src_ref=src, dst_ref=dst, send_sem=send, recv_sem=recv, device_id=where, device_id_type=MESH)

    def slot(k):
        return pl.ds(k * piece, piece)

    barrier = pltpu.get_barrier_semaphore()
    for s in range(1, n_cp):
        pl.semaphore_signal(barrier, inc=1, device_id={'cp': mate(s)}, device_id_type=MESH)
    for step in (1, n_pl - 1):
        pl.semaphore_signal(barrier, inc=1, device_id={'cpo': lax.rem(z + step, n_pl)}, device_id_type=MESH)
    pl.semaphore_wait(barrier, n_cp + 1)

    def q_copies(j, s):
        out = []
        for t, src in enumerate((q_in, g_in)):
            dst = gat.at[j, t, pl.ds(s * part, part), :]
            if s == 0:
                out.append(pltpu.make_async_copy(src.at[j, c], dst, q_r.at[j, 0, t]))
            else:
                out.append(remote(src.at[j, mate(s)], dst, q_s.at[s, t], q_r.at[j, s, t], cp=mate(s)))
        return out

    def q_start(j, carry):
        for s in range(n_cp):
            for copy in q_copies(j, s):
                copy.start()
        return carry

    def kv_copies(s):
        out = []
        for t, src in enumerate((k_in, v_in)):
            dst = kv_scr.at[t, pl.ds(pl.multiple_of(c * key_rows, 64), key_rows), :]
            if s == 0:
                out.append(pltpu.make_async_copy(src.at[c], dst, kv_r.at[0, t]))
            else:
                out.append(remote(src.at[mate(s)], dst, kv_s.at[s, t], kv_r.at[s, t], cp=mate(s)))
        return out

    def st_copy(s):
        if s == 0:
            return pltpu.make_async_copy(st.at[c], st_scr.at[0, 0], st_r.at[0])
        return remote(st.at[mate(s)], st_scr.at[0, s], st_s.at[s], st_r.at[s], cp=mate(s))

    lax.fori_loop(0, FIRST, q_start, 0)
    for s in range(n_cp):
        st_copy(s).start()
    for s in range(n_cp):
        for copy in kv_copies(s):
            copy.start()
    lax.fori_loop(FIRST, n_slices, q_start, 0)

    def ups(h):
        return (z < far) & (z >= h - 1)

    def downs(h):
        return (z >= 1) & (z <= n_pl - h)

    def q_hop(j, h, up):
        a, b = (h - 1, h) if up else ((n_pl - h + 1) % n_pl, n_pl - h)
        d = 0 if up else 1
        return remote(gat.at[j, :, slot(a), :], gat.at[j, :, slot(b), :], ag_s.at[d, h - 1], ag_r.at[j, b], cpo=z + 1 if up else z - 1)

    def st_hop(h, up):
        a, b = (h - 1, h) if up else ((n_pl - h + 1) % n_pl, n_pl - h)
        d = 0 if up else 1
        return remote(st_scr.at[a], st_scr.at[b], sz_s.at[d, h - 1], sz_r.at[b], cpo=z + 1 if up else z - 1)

    def send_hop(make, h):
        @pl.when(ups(h))
        def _():
            make(h, True).start()

        @pl.when(downs(h))
        def _():
            make(h, False).start()

    def wait_hop(make, h):
        @pl.when(z >= h)
        def _():
            make(h, True).wait_recv()

        @pl.when(z <= far - h)
        def _():
            make(h, False).wait_recv()

    def ag_first(j):
        for s in range(n_cp):
            for copy in q_copies(j, s):
                copy.wait() if s == 0 else copy.wait_recv()
        send_hop(lambda h, up: q_hop(j, h, up), 1)

    def ag_next(j, h):
        wait_hop(lambda h, up: q_hop(j, h, up), h - 1)
        send_hop(lambda h, up: q_hop(j, h, up), h)

    def ag_service(t, due):
        for h in range(1, n_pl):
            jj = t + AHEAD - (h - 1)

            @pl.when(due & (jj < n_slices))
            def _():
                ag_first(jj) if h == 1 else ag_next(jj, h)

    def rs_copy(j, s, up):
        k = s if up else n_pl - s
        d = 0 if up else 1
        dst = (ru if up else rd).at[j, s - 1]
        return remote(dqp.at[j, slot(k), :], dst, rs_s.at[d, s - 1], rs_r.at[d, j, s - 1], cpo=z + 1 if up else z - 1)

    def rs_step(j, s):
        if s > 1:
            @pl.when((z >= 1) & (z <= s - 1))
            def _():
                rs_copy(j, s - 1, True).wait_recv()
                dqp[j, slot(s), :] += ru[j, s - 2]

            @pl.when((z >= n_pl - s) & (z <= far - 1))
            def _():
                rs_copy(j, s - 1, False).wait_recv()
                dqp[j, slot(n_pl - s), :] += rd[j, s - 2]

        @pl.when(z <= s - 1)
        def _():
            rs_copy(j, s, True).start()

        @pl.when(z >= n_pl - s)
        def _():
            rs_copy(j, s, False).start()

    def dq_copy(j, s):
        src = dqb.at[j, pl.ds(s * part, part), :]
        if s == 0:
            return pltpu.make_async_copy(src, dq_out.at[j, c], dq_r.at[0])
        return remote(src, dq_out.at[j, c], dq_s.at[s], dq_r.at[s], cp=mate(s))

    def rs_final(j):
        @pl.when(z >= 1)
        def _():
            rs_copy(j, far, True).wait_recv()
            dqp[j, slot(0), :] += ru[j, far - 1]

        @pl.when(z <= far - 1)
        def _():
            rs_copy(j, far, False).wait_recv()
            dqp[j, slot(0), :] += rd[j, far - 1]

        dqb[j] = (dqp[j, slot(0), :] * scale).astype(jnp.bfloat16)
        for s in range(n_cp):
            dq_copy(j, s).start()

    def rs_service(u, due, low, high):
        for s in range(1, n_pl + 1):
            jj = u - s

            @pl.when(due & (jj >= low) & (jj < high))
            def _():
                rs_step(jj, s) if s < n_pl else rs_final(jj)

    def compute(j, low, high, fresh):
        @pl.when(fresh)
        def _():
            dqp[j] = jnp.zeros(dqp.shape[1:], jnp.float32)

        cols16 = [st_scr[k, s, pl.ds(2 * j, 2), :] for k in range(n_pl) for s in range(n_cp)]
        stat_t = jnp.concatenate(cols16, axis=0).T
        for i in range(n_pl * n_cp):
            rr = pl.ds(i * part, part)
            l_scr[rr, :] = jnp.broadcast_to(stat_t[:part, 2 * i:2 * i + 1] * LOG2E, (part, 128))
            d_scr[rr, :] = jnp.broadcast_to(stat_t[:part, 2 * i + 1:2 * i + 2], (part, 128))

        @pl.when(fresh)
        def _():
            turned[j, 0] = gat[j, 0].T
            turned[j, 1] = gat[j, 1].T


        def scores(r, kt, vt):
            rr = pl.ds(r * SUB, SUB)
            s = jnp.dot(gat[j, 0, rr, :], kt, preferred_element_type=jnp.float32)
            dp = jnp.dot(gat[j, 1, rr, :], vt, preferred_element_type=jnp.float32)
            return s, dp

        def probs(r, s, dp, masked):
            rr = pl.ds(r * SUB, SUB)
            lb = l_scr[rr, :]
            db = d_scr[rr, :]
            lb = jnp.concatenate([lb, lb], axis=1)
            db = jnp.concatenate([db, db], axis=1)
            p = jnp.exp2(s * (scale * LOG2E) - lb)
            if masked:
                pos = qpos[rr, :]
                pos = jnp.concatenate([pos, pos], axis=1)
                key = lax.broadcasted_iota(jnp.int32, (SUB, KEY_BLOCK), 1)
                p = jnp.where(key <= pos, p, 0.0)
            return p.astype(jnp.bfloat16), (p * (dp - db)).astype(jnp.bfloat16)

        def blocks(first, count, masked=False):
            cols = [pl.ds(pl.multiple_of((first + n) * KEY_BLOCK, KEY_BLOCK), KEY_BLOCK) for n in range(count)]
            n_sub = rows // SUB
            held = None
            for i in range(count * n_sub + 1):
                if i < count * n_sub:
                    here = cols[i // n_sub]
                    s, dp = scores(i % n_sub, kt_scr[:, here], vt_scr[:, here])
                if held is not None:
                    r = (i - 1) % n_sub
                    there = cols[(i - 1) // n_sub]
                    q = pl.ds(r * SUB, SUB)
                    p, ds = held
                    av = jnp.dot(turned[j, 1, :, q], p, preferred_element_type=jnp.float32)
                    ak = jnp.dot(turned[j, 0, :, q], ds, preferred_element_type=jnp.float32)
                    acc_v = av if r == 0 else acc_v + av
                    acc_k = ak if r == 0 else acc_k + ak
                    dqp[j, q, :] += jnp.dot(ds, kv_scr[0, there, :], preferred_element_type=jnp.float32)
                    if r == n_sub - 1:
                        dv_scr[:, there] += acc_v
                        dk_scr[:, there] += acc_k
                if i < count * n_sub:
                    held = probs(i % n_sub, s, dp, masked)

        edge = lax.div(z, far) * (n_pref_last + j - n_blocks) + n_blocks
        top = lax.min(high, edge)
        many = lax.div(top - low, TOGETHER)
        many = lax.max(many, 0)
        mid = low + many * TOGETHER

        def step(n, carry):
            blocks(low + n * TOGETHER, TOGETHER)
            return carry

        lax.fori_loop(0, many, step, 0)

        def single(b, carry):
            blocks(b, 1)
            return carry

        lax.fori_loop(mid, top, single, 0)

        @pl.when((edge >= low) & (edge < high))
        def _():
            blocks(edge, 1, True)

    dk_scr[...] = jnp.zeros_like(dk_scr)
    dv_scr[...] = jnp.zeros_like(dv_scr)
    for j in range(FIRST):
        ag_first(j)
    for s in range(n_cp):
        copy = st_copy(s)
        copy.wait() if s == 0 else copy.wait_recv()
    send_hop(st_hop, 1)
    for h in range(2, n_pl):
        for j in range(FIRST):
            ag_next(j, h)
        wait_hop(st_hop, h - 1)
        send_hop(st_hop, h)
    y = lax.div(c, 2)
    own = (y * ((n_blocks + 1) // 2), n_blocks // 2 + y * (n_blocks - n_blocks // 2))
    other = ((1 - y) * (n_blocks // 2), n_blocks - y * (n_blocks // 2))

    def turn(b, carry):
        cols = pl.ds(pl.multiple_of(b * KEY_BLOCK, KEY_BLOCK), KEY_BLOCK)
        kt_scr[:, cols] = kv_scr[0, cols, :].T
        vt_scr[:, cols] = kv_scr[1, cols, :].T
        return carry

    for copy in kv_copies(0):
        copy.wait()
    for copy in kv_copies(1):
        copy.wait_recv()
    lax.fori_loop(own[0], own[1], turn, 0)
    wait_hop(st_hop, far)

    def home(src, out, s, n):
        place = src.at[pl.ds(pl.multiple_of(mate(s) * key_rows, 64), key_rows), :]
        if s == 0:
            return pltpu.make_async_copy(place, out.at[c], dk_r.at[n, 0])
        return remote(place, out.at[c], dk_s.at[n, s], dk_r.at[n, s], cp=mate(s))

    pairs = ((dv_scr, dvo, dv_out, 1.0), (dk_scr, dko, dk_out, scale))

    def go_home(span, mates):
        for n, (acc, held, out, factor) in enumerate(pairs):
            def turn_back(b, carry):
                cols = pl.ds(pl.multiple_of(b * KEY_BLOCK, KEY_BLOCK), KEY_BLOCK)
                held[cols, :] = acc[:, cols].T * factor
                return carry

            lax.fori_loop(span[0], span[1], turn_back, 0)
            for s in mates:
                home(held, out, s, n).start()

    half = n_slices // 2

    def item(i, carry):
        early = i < 2 * half
        late = i >= half + n_slices
        j = jnp.where(i < 2, i, jnp.where(i < 4, i - 2, jnp.where(early, lax.div(i, 2), jnp.where(late, i - n_slices, i - half))))
        is_own = jnp.where(i < 2, 1, jnp.where(i < 4, 0, jnp.where(early, 1 - lax.rem(i, 2), jnp.where(late, 1, 0))))
        is_first = jnp.where(i < 2, 1, jnp.where(i < 4, 0, jnp.where(early, 1 - lax.rem(i, 2), jnp.where(late, 0, 1))))
        low = is_own * own[0] + (1 - is_own) * other[0]
        high = is_own * own[1] + (1 - is_own) * other[1]
        even = lax.rem(i, 2) == 0

        for h in range(1, n_pl):
            for jj in range(FIRST, min(AHEAD - (h - 1), n_slices)):
                @pl.when(i == 1)
                def _():
                    ag_first(jj) if h == 1 else ag_next(jj, h)

        ag_service(jnp.where(i < 8, lax.div(i, 2) - 1, i - 5), ((i >= 2) & even) | (i > 8))

        @pl.when(i == 2)
        def _():
            for s in range(2, n_cp):
                for copy in kv_copies(s):
                    copy.wait_recv()
            lax.fori_loop(other[0], other[1], turn, 0)

        rs_service(
            jnp.where(i <= 2 * half, lax.div(i, 2), i - half),
            (i == 3) | ((i >= 4) & (i <= 2 * half) & even) | ((i > 2 * half) & (i < 2 * half + n_pl)), 0, half)
        rs_service(i - n_slices, i > half + n_slices, half, n_slices)

        @pl.when(i == half + n_slices)
        def _():
            go_home(other, (2, 3))

        @pl.when(is_first == 1)
        def _():
            wait_hop(lambda h, up: q_hop(j, h, up), far)

        compute(j, low, high, is_first == 1)
        return carry

    lax.fori_loop(0, 2 * n_slices, item, 0)
    rs_service(n_slices, z >= 0, half, n_slices)
    go_home(own, (1, 0))

    def flush(u, carry):
        rs_service(u, u >= 0, half, n_slices)
        return carry

    lax.fori_loop(n_slices + 1, n_slices + n_pl, flush, 0)

    for s in range(n_cp):
        whole = dqb.at[:, pl.ds(s * part, part), :]
        if s == 0:
            pltpu.make_async_copy(whole, dq_out.at[:, c], dq_r.at[0]).wait()
        else:
            remote(whole, dq_out.at[:, mate(s)], dq_s.at[s], dq_r.at[s], cp=mate(s)).wait()
            for t, src in enumerate((q_in, g_in)):
                remote(src.at[:, mate(s)], gat.at[:, t, pl.ds(s * part, part), :], q_s.at[s, t], q_r.at[0, s, t], cp=mate(s)).wait_send()
            for copy in kv_copies(s):
                copy.wait_send()
            st_copy(s).wait_send()
        for n, (acc, held, out, factor) in enumerate(pairs):
            home(held, out, s, n).wait()
    for h in range(1, n_pl):
        for up in (True, False):
            cond = ups(h) if up else downs(h)

            @pl.when(cond)
            def _():
                d = 0 if up else 1
                whole = gat.at[:, :, slot(0), :]
                remote(whole, whole, ag_s.at[d, h - 1], ag_r.at[0, 1], cpo=z + 1 if up else z - 1).wait_send()
                st_hop(h, up).wait_send()

            cond = (z <= h - 1) if up else (z >= n_pl - h)

            @pl.when(cond)
            def _():
                d = 0 if up else 1
                whole = dqp.at[:, slot(0), :]
                remote(whole, whole, rs_s.at[d, h - 1], rs_r.at[d, 0, 0], cpo=z + 1 if up else z - 1).wait_send()


def interleave_kernel(dk_ref, dv_ref, dk_out, dv_out):
    heads, n, _ = dk_ref.shape
    for src, dst in ((dk_ref, dk_out), (dv_ref, dv_out)):
        for h in range(heads):
            dst[pl.ds(h, n, stride=heads), :] = src[h]


def solution(mesh):
    n_cpo = mesh.shape['cpo']
    n_cp = mesh.shape['cp']
    row_spec = P(None, CP_AXES, 'heads', None)
    stat_spec = P(None, CP_AXES, 'heads')
    key_spec = P(CP_AXES, 'heads', None)

    def local_grads(queries, attn_out, grad_out, log_sum_exp, key_cache, value_cache):
        n_slices, rows_dev, q_heads, head_dim = queries.shape
        key_rows, kv_heads, _ = key_cache.shape
        group = q_heads // kv_heads
        slice_len = rows_dev * n_cp * n_cpo
        plane_keys = key_rows * n_cp
        prefix = plane_keys * n_cpo - n_slices * slice_len
        n_pref_last = (prefix - plane_keys * (n_cpo - 1)) // KEY_BLOCK
        scale = head_dim ** -0.5
        part = rows_dev * group
        piece = n_cp * part
        rows = n_cpo * piece
        bf, f32 = jnp.bfloat16, jnp.float32
        z = lax.axis_index('cpo')
        c = lax.axis_index('cp')

        delta = jnp.sum(grad_out.astype(f32) * attn_out.astype(f32), axis=-1)
        st = jnp.stack([log_sum_exp, delta], axis=1).transpose(3, 0, 1, 2).reshape(kv_heads, group, n_slices, 2, rows_dev)
        st = st.transpose(0, 2, 3, 1, 4).reshape(kv_heads, n_slices * 2, part)
        st = jnp.pad(st, ((0, 0), (0, -(n_slices * 2) % 8), (0, 128 - part)))

        def by_head(x):
            return jnp.transpose(x, (0, 2, 1, 3)).reshape(n_slices, kv_heads, part, head_dim)

        keys, values = (jnp.transpose(x, (1, 0, 2)) for x in (key_cache, value_cache))

        r = jnp.arange(rows)
        plane = (z - r // piece) % n_cpo
        tok = plane * n_cp * rows_dev + (c ^ ((r % piece) // part)) * rows_dev + r % rows_dev
        tok = jnp.where(z == n_cpo - 1, tok, slice_len)
        qpos = jnp.broadcast_to(tok[:, None], (rows, 128)).astype(jnp.int32)

        any_spec = pl.BlockSpec(memory_space=pl.ANY)
        vmem = pl.BlockSpec(memory_space=pltpu.VMEM)
        dma = pltpu.SemaphoreType.DMA
        dq, dk, dv = pl.pallas_call(
            functools.partial(attention_kernel, n_cpo, n_cp, n_pref_last, scale),
            out_shape=[
                jax.ShapeDtypeStruct((n_slices, kv_heads, part, head_dim), bf),
                jax.ShapeDtypeStruct((kv_heads, key_rows, head_dim), f32),
                jax.ShapeDtypeStruct((kv_heads, key_rows, head_dim), f32),
            ],
            in_specs=[any_spec] * 5 + [vmem],
            out_specs=[any_spec] * 3,
            scratch_shapes=[
                pltpu.VMEM((n_slices, 2, rows, head_dim), bf),
                pltpu.VMEM((2, plane_keys, head_dim), bf),
                pltpu.VMEM((head_dim, plane_keys), bf),
                pltpu.VMEM((head_dim, plane_keys), bf),
                pltpu.VMEM((n_cpo, n_cp) + st.shape[1:], f32),
                pltpu.VMEM((n_slices, rows, head_dim), f32),
                pltpu.VMEM((n_slices, n_cpo - 1, piece, head_dim), f32),
                pltpu.VMEM((n_slices, n_cpo - 1, piece, head_dim), f32),
                pltpu.VMEM((n_slices, piece, head_dim), bf),
                pltpu.VMEM((head_dim, plane_keys), f32),
                pltpu.VMEM((head_dim, plane_keys), f32),
                pltpu.VMEM((plane_keys, head_dim), f32),
                pltpu.VMEM((plane_keys, head_dim), f32),
                pltpu.VMEM((n_slices, 2, head_dim, rows), bf),
                pltpu.VMEM((rows, 128), f32),
                pltpu.VMEM((rows, 128), f32),
                dma((n_cp, 2)), dma((n_slices, n_cp, 2)),
                dma((n_cp, 2)), dma((n_cp, 2)),
                dma((n_cp,)), dma((n_cp,)),
                dma((2, n_cpo - 1)), dma((n_cpo,)),
                dma((2, n_cpo - 1)), dma((n_slices, n_cpo)),
                dma((2, n_cpo - 1)), dma((2, n_slices, n_cpo - 1)),
                dma((n_cp,)), dma((n_cp,)),
                dma((2, n_cp)), dma((2, n_cp)),
            ],
            compiler_params=pltpu.CompilerParams(vmem_limit_bytes=63 * 1024 * 1024, collective_id=0, has_side_effects=True),
            name='attention_backward',
        )(by_head(queries), by_head(grad_out), keys, values, st, qpos)

        block_rows = key_rows // 4
        dk, dv = pl.pallas_call(
            interleave_kernel,
            grid=(4,),
            out_shape=[jax.ShapeDtypeStruct((key_rows * kv_heads, head_dim), f32)] * 2,
            in_specs=[pl.BlockSpec((kv_heads, block_rows, head_dim), lambda b: (0, b, 0))] * 2,
            out_specs=[pl.BlockSpec((block_rows * kv_heads, head_dim), lambda b: (b, 0))] * 2,
            compiler_params=pltpu.CompilerParams(vmem_limit_bytes=24 * 1024 * 1024),
            name='interleave',
        )(dk, dv)
        grad_query = jnp.transpose(dq.reshape(n_slices, q_heads, rows_dev, head_dim), (0, 2, 1, 3))
        return grad_query, dk.reshape(key_cache.shape), dv.reshape(key_cache.shape)

    return jax.shard_map(local_grads, mesh=mesh, in_specs=(row_spec, row_spec, row_spec, stat_spec, key_spec, key_spec), out_specs=(row_spec, key_spec, key_spec), check_vma=False)
```
